8 devices in a mesh: dp: 1 (over z), sp: 2 (over y), tp: 4 (over x, core).
Axes of the slice: x: 2, y: 2, z: 1, core: 2. Of those that a mesh axis runs over, the one named last changes fastest.
Arguments:
- latents: bfloat16 [8, 784, 512], P('dp')
- queries: bfloat16 [8, 16384, 704], P('dp', 'sp')
- lat_ln1: float32 [512], replicated
- lat_wq: bfloat16 [512, 8, 64], P(None, 'tp')
- lat_wk: bfloat16 [512, 8, 64], P(None, 'tp')
- lat_wv: bfloat16 [512, 8, 64], P(None, 'tp')
- lat_wo: bfloat16 [8, 64, 512], P('tp')
- lat_ln2: float32 [512], replicated
- lat_up: bfloat16 [512, 512], P(None, 'tp')
- lat_down: bfloat16 [512, 512], P('tp')
- dec_lnq: float32 [704], replicated
- dec_lnkv: float32 [512], replicated
- dec_wq: bfloat16 [704, 512], replicated
- dec_wk: bfloat16 [512, 512], replicated
- dec_wv: bfloat16 [512, 512], replicated
- dec_wo: bfloat16 [512, 512], replicated
- dec_ln: float32 [512], replicated
- dec_up: bfloat16 [512, 512], replicated
- dec_down: bfloat16 [512, 512], replicated
- dec_out: bfloat16 [512, 512], replicated
Outputs:
- output: bfloat16 [8, 16384, 512], P('dp', 'sp')
All inputs are finite; a program needn't handle non-finite values.
Results may differ from the reference program's by a relative error of at most 0.0179948.
Values are sent between devices in bfloat16 or wider.
A program may use at most 1 GiB of HBM per device.

```python
import jax
import jax.numpy as jnp
from jax import lax

BATCH = 8
LATENTS = 784
WIDTH = 512
HEADS = 8
HEAD_DIM = 64
MLP_WIDTH = 512
QUERY_CH = 704
DEC_WIDTH = 512
OUT_CH = 512
QUERIES = 16384
QUERY_BLOCK = 512
LN_EPS = 1e-5


def layer_norm(rows_in, gain_vec):
    widened = rows_in.astype(jnp.float32)
    row_mean = jnp.mean(widened, axis=-1, keepdims=True)
    row_var = jnp.mean(jnp.square(widened - row_mean), axis=-1, keepdims=True)
    return ((widened - row_mean) * lax.rsqrt(row_var + LN_EPS) * gain_vec).astype(jnp.bfloat16)


def setup_inputs(seed: int = 0, part: int = 0) -> dict:
    shared = jax.random.split(jax.random.key(seed), 18)
    own_keys = jax.random.split(jax.random.fold_in(jax.random.key(seed + 1), part), 2)

    def draw_normal(rng_key, arr_shape, std_scale):
        return (jax.random.normal(rng_key, arr_shape, jnp.float32) * std_scale).astype(jnp.bfloat16)

    def draw_gain(rng_key, vec_len):
        return 1.0 + 0.3 * jax.random.normal(rng_key, (vec_len,), jnp.float32)

    head_shape = (WIDTH, HEADS, HEAD_DIM)
    return {
        "latents": draw_normal(own_keys[0], (BATCH, LATENTS, WIDTH), 1.0),
        "queries": draw_normal(own_keys[1], (BATCH, QUERIES, QUERY_CH), 1.0),
        "lat_ln1": draw_gain(shared[0], WIDTH),
        "lat_wq": draw_normal(shared[1], head_shape, 1.5 * WIDTH ** -0.5),
        "lat_wk": draw_normal(shared[2], head_shape, 1.5 * WIDTH ** -0.5),
        "lat_wv": draw_normal(shared[3], head_shape, WIDTH ** -0.5),
        "lat_wo": draw_normal(shared[4], (HEADS, HEAD_DIM, WIDTH), (HEADS * HEAD_DIM) ** -0.5),
        "lat_ln2": draw_gain(shared[5], WIDTH),
        "lat_up": draw_normal(shared[6], (WIDTH, MLP_WIDTH), WIDTH ** -0.5),
        "lat_down": draw_normal(shared[7], (MLP_WIDTH, WIDTH), MLP_WIDTH ** -0.5),
        "dec_lnq": draw_gain(shared[8], QUERY_CH),
        "dec_lnkv": draw_gain(shared[9], WIDTH),
        "dec_wq": draw_normal(shared[10], (QUERY_CH, DEC_WIDTH), 1.5 * QUERY_CH ** -0.5),
        "dec_wk": draw_normal(shared[11], (WIDTH, DEC_WIDTH), 1.5 * WIDTH ** -0.5),
        "dec_wv": draw_normal(shared[12], (WIDTH, DEC_WIDTH), 2.0 * WIDTH ** -0.5),
        "dec_wo": draw_normal(shared[13], (DEC_WIDTH, DEC_WIDTH), 1.5 * DEC_WIDTH ** -0.5),
        "dec_ln": draw_gain(shared[14], DEC_WIDTH),
        "dec_up": draw_normal(shared[15], (DEC_WIDTH, DEC_WIDTH), DEC_WIDTH ** -0.5),
        "dec_down": draw_normal(shared[16], (DEC_WIDTH, DEC_WIDTH), DEC_WIDTH ** -0.5),
        "dec_out": draw_normal(shared[17], (DEC_WIDTH, OUT_CH), DEC_WIDTH ** -0.5),
    }


def latent_layer(z_one, lat_ln1, lat_wq, lat_wk, lat_wv, lat_wo, lat_ln2, lat_up, lat_down):
    normed = layer_norm(z_one, lat_ln1).astype(jnp.float32)
    q_heads = jnp.einsum("nd,dhe->nhe", normed, lat_wq.astype(jnp.float32)).astype(jnp.bfloat16)
    k_heads = jnp.einsum("nd,dhe->nhe", normed, lat_wk.astype(jnp.float32)).astype(jnp.bfloat16)
    v_heads = jnp.einsum("nd,dhe->nhe", normed, lat_wv.astype(jnp.float32)).astype(jnp.bfloat16)
    scores = jnp.einsum("qhe,khe->hqk", q_heads.astype(jnp.float32), k_heads.astype(jnp.float32)) * HEAD_DIM ** -0.5
    attn_probs = jax.nn.softmax(scores, axis=-1).astype(jnp.bfloat16)
    context = jnp.einsum("hqk,khe->qhe", attn_probs.astype(jnp.float32), v_heads.astype(jnp.float32)).astype(jnp.bfloat16)
    attn_out = jnp.einsum("qhe,hed->qd", context.astype(jnp.float32), lat_wo.astype(jnp.float32))
    z_mid = (z_one.astype(jnp.float32) + attn_out).astype(jnp.bfloat16)
    hidden = jax.nn.gelu(jnp.dot(layer_norm(z_mid, lat_ln2), lat_up, preferred_element_type=jnp.float32), approximate=False).astype(jnp.bfloat16)
    return (z_mid.astype(jnp.float32) + jnp.dot(hidden, lat_down, preferred_element_type=jnp.float32)).astype(jnp.bfloat16)


def decode_block(q_block, all_keys, all_values, dec_lnq, dec_wq, dec_wo, dec_ln, dec_up, dec_down, dec_out):
    q_proj = jnp.dot(layer_norm(q_block, dec_lnq), dec_wq, preferred_element_type=jnp.float32).astype(jnp.bfloat16)
    scores = jnp.dot(q_proj, all_keys.T, preferred_element_type=jnp.float32) * DEC_WIDTH ** -0.5
    attn_probs = jax.nn.softmax(scores, axis=-1).astype(jnp.bfloat16)
    context = jnp.dot(attn_probs, all_values, preferred_element_type=jnp.float32).astype(jnp.bfloat16)
    mixed_rows = (q_proj.astype(jnp.float32) + jnp.dot(context, dec_wo, preferred_element_type=jnp.float32)).astype(jnp.bfloat16)
    hidden = jax.nn.gelu(jnp.dot(layer_norm(mixed_rows, dec_ln), dec_up, preferred_element_type=jnp.float32), approximate=False).astype(jnp.bfloat16)
    final_rows = (mixed_rows.astype(jnp.float32) + jnp.dot(hidden, dec_down, preferred_element_type=jnp.float32)).astype(jnp.bfloat16)
    return jnp.dot(final_rows, dec_out, preferred_element_type=jnp.float32).astype(jnp.bfloat16)


def reference(latents, queries, lat_ln1, lat_wq, lat_wk, lat_wv, lat_wo, lat_ln2, lat_up, lat_down, dec_lnq, dec_lnkv, dec_wq, dec_wk, dec_wv, dec_wo, dec_ln, dec_up, dec_down, dec_out):
    def one_item(item_pair):
        z_one, q_one = item_pair
        z_new = latent_layer(z_one, lat_ln1, lat_wq, lat_wk, lat_wv, lat_wo, lat_ln2, lat_up, lat_down)
        kv_in = layer_norm(z_new, dec_lnkv)
        all_keys = jnp.dot(kv_in, dec_wk, preferred_element_type=jnp.float32).astype(jnp.bfloat16)
        all_values = jnp.dot(kv_in, dec_wv, preferred_element_type=jnp.float32).astype(jnp.bfloat16)
        query_blocks = q_one.reshape(QUERIES // QUERY_BLOCK, QUERY_BLOCK, QUERY_CH)
        out_blocks = lax.map(lambda q_block: decode_block(q_block, all_keys, all_values, dec_lnq, dec_wq, dec_wo, dec_ln, dec_up, dec_down, dec_out), query_blocks)
        return out_blocks.reshape(QUERIES, OUT_CH)
    return lax.map(one_item, (latents, queries))
```

```python
import functools

import jax
import jax.numpy as jnp
from jax import lax
from jax.experimental import pallas as pl
from jax.experimental.pallas import tpu as pltpu
from jax.sharding import PartitionSpec as P


F32, BF16 = jnp.float32, jnp.bfloat16
EPS = 1e-5
LOG2E = 1.4426950408889634
CORE = [(0, 1), (1, 0), (2, 3), (3, 2)]
CHIP = [(0, 2), (2, 0), (1, 3), (3, 1)]
T = 1024


def dot(a, b):
    return jnp.dot(a, b, preferred_element_type=F32)


def dot_t(a, b):
    return lax.dot_general(a, b, (((0,), (0,)), ((), ())), preferred_element_type=F32)


def ln_t(cols, gain):
    x = cols.astype(F32)
    n = x.shape[0]
    mean = jnp.sum(x, axis=0, keepdims=True) * (1.0 / n)
    d = x - mean
    var = jnp.sum(d * d, axis=0, keepdims=True) * (1.0 / n)
    return (d * lax.rsqrt(var + EPS) * gain).astype(BF16)


def gelu(h):
    return (0.5 * h * (1.0 + lax.erf(h * (0.5 ** 0.5)))).astype(BF16)


def attend(scores, values_t, scale):
    c = scale * LOG2E
    m = jnp.max(scores, axis=0, keepdims=True) * c
    p = jnp.exp2(scores * c - m)
    inv = 1.0 / jnp.sum(p, axis=0, keepdims=True)
    return dot(values_t, p.astype(BF16)) * inv


def keys_values(z_t, gkv, wk, wv, wo):
    a = ln_t(z_t, gkv)
    keys = dot_t(a, wk).astype(BF16)
    vals_t = dot_t(wv, a).astype(BF16)
    return keys, dot_t(wo, vals_t).astype(BF16)


def latent_kernel(z_ref, w_ref, g1, g2, gkv, wk, wv, wo, z_out, k_out, vw_out, c_s):
    n_shard, head = w_ref.shape[0], 64
    z = z_ref[...]
    a = ln_t(z, g1[...])
    width = n_shard * 128

    def part(i):
        return w_ref[:, i].reshape(width, w_ref.shape[3])

    q = dot(part(0), a).astype(BF16)
    k = dot(part(1), a).astype(BF16)
    v = dot(part(2), a).astype(BF16)
    for h in range(width // head):
        rows = slice(h * head, (h + 1) * head)
        c_s[rows, :] = attend(dot_t(k[rows], q[rows]), v[rows], head ** -0.5).astype(BF16)
    z1 = (z.astype(F32) + dot_t(part(3), c_s[...])).astype(BF16)
    hid = gelu(dot(part(4), ln_t(z1, g2[...])))
    z2 = (z1.astype(F32) + dot_t(part(5), hid)).astype(BF16)
    z_out[...] = z2
    keys, vw = keys_values(z2, gkv[...], wk[...], wv[...], wo[...])
    k_out[...] = keys
    vw_out[...] = vw


def kv_kernel(z_ref, gkv, wk, wv, wo, k_out, vw_out):
    keys, vw = keys_values(z_ref[...], gkv[...], wk[...], wv[...], wo[...])
    k_out[...] = keys
    vw_out[...] = vw


def decode_cols(q_cols, keys, vw_t, gq, wq_t, gd, wup_t, wdn_t, wout):
    qd = dot(wq_t, ln_t(q_cols, gq)).astype(BF16)
    o = attend(dot(keys, qd), vw_t, keys.shape[1] ** -0.5)
    x = (qd.astype(F32) + o).astype(BF16)
    hid = gelu(dot(wup_t, ln_t(x, gd)))
    x2 = (x.astype(F32) + dot(wdn_t, hid)).astype(BF16)
    return dot_t(x2, wout).astype(BF16)


def stage_kernel(n_steps, n_sendx, n_recv, has_y, decode, *refs):
    refs = list(refs)
    tab = refs.pop(0)
    ins = [refs.pop(0) for _ in range(9 if decode else 0)]
    recv = [refs.pop(0) for _ in range(n_recv)]
    if has_y:
        refs.pop(0)
    y_ref = refs.pop(0)
    send_ref = refs.pop(0) if decode else None
    sendx_ref = refs.pop(0) if n_sendx else None
    i = pl.program_id(0)
    if decode:
        y_s, sem_y, sem_s, sem_x = refs.pop(0), refs.pop(0), refs.pop(0), refs.pop(0)
    sem_r = refs.pop(0) if n_recv else None

    def recv_copy(r):
        rows = recv[r].shape[0]
        start = pl.multiple_of(tab[3 + 2 * r, i], 8)
        return pltpu.make_async_copy(recv[r], y_ref.at[tab[2 + 2 * r, i], pl.ds(start, rows), :], sem_r.at[r])

    for r in range(n_recv):
        recv_copy(r).start()

    if decode:
        slot = lax.rem(i, 2)

        def out_copies(step, sl):
            start = pl.multiple_of(tab[1, step] * T, T)
            at = pl.multiple_of(step * T, T)
            copies = [
                pltpu.make_async_copy(y_s.at[sl], y_ref.at[tab[0, step], pl.ds(start, T), :], sem_y.at[sl]),
                pltpu.make_async_copy(y_s.at[sl], send_ref.at[pl.ds(at, T), :], sem_s.at[sl]),
            ]
            return copies

        def x_copy(step, sl):
            at = pl.multiple_of(step * T, T)
            return pltpu.make_async_copy(y_s.at[sl], sendx_ref.at[pl.ds(at, T), :], sem_x.at[sl])

        def finish(step, sl):
            for c in out_copies(step, sl):
                c.wait()
            if n_sendx:
                @pl.when(step < n_sendx)
                def _():
                    x_copy(step, sl).wait()

        @pl.when(i >= 2)
        def _():
            finish(i - 2, slot)

        x_ref, k, vw, gq, wq, gd, wup, wdn, wout = ins
        y_s[slot] = decode_cols(x_ref[0], k[...], vw[...], gq[...], wq[...], gd[...], wup[...], wdn[...], wout[...])
        for c in out_copies(i, slot):
            c.start()
        if n_sendx:
            @pl.when(i < n_sendx)
            def _():
                x_copy(i, slot).start()

        @pl.when(i == n_steps - 1)
        def _():
            if n_steps > 1:
                finish(i - 1, 1 - slot)
            finish(i, slot)

    for r in range(n_recv):
        recv_copy(r).wait()


def full_spec(arr):
    return pl.BlockSpec(arr.shape, lambda i, tab: (0,) * arr.ndim)


ANY = pl.BlockSpec(memory_space=pl.ANY)
PARAMS = functools.partial(pltpu.CompilerParams, vmem_limit_bytes=56 * 2 ** 20)


def solution(mesh):
    whole_vec, whole_mat, head_split = P(None), P(None, None), P(None, "tp", None)
    in_specs = (P("dp", None, None), P("dp", "sp", None), whole_vec, head_split, head_split, head_split, P("tp", None, None), whole_vec, P(None, "tp"), P("tp", None), whole_vec, whole_vec, whole_mat, whole_mat, whole_mat, whole_mat, whole_vec, whole_mat, whole_mat, whole_mat)

    def stage(name, y, y_shape, blocks, queries_t, kv, weights, recvs, n_sendx=0, steps=None):
        n = len(blocks) if blocks else steps
        item_rows = [b[0] for b in blocks] or [0] * n
        blk_rows = [b[1] for b in blocks] or [0] * n
        table = [item_rows, blk_rows]
        for _, where in recvs:
            table += [[w[0] for w in where], [w[1] for w in where]]
        tab = jnp.stack([jnp.stack([jnp.asarray(v, jnp.int32) for v in row]) for row in table])
        args, specs = [], []
        if blocks:
            args += [queries_t, *kv, *weights]
            specs += [pl.BlockSpec((1, queries_t.shape[1], T), lambda i, tab: (tab[0, i], 0, tab[1, i]))]
            specs += [full_spec(a) for a in (*kv, *weights)]
        for rows, _ in recvs:
            args.append(rows)
            specs.append(pl.BlockSpec((rows.shape[0] // n, rows.shape[1]), lambda i, tab: (i, 0)))
        aliases = {}
        if y is not None:
            aliases = {1 + len(args): 0}
            args.append(y)
            specs.append(ANY)
        width = y_shape[2]
        outs, out_specs, scratch = [jax.ShapeDtypeStruct(y_shape, BF16)], [ANY], []
        if blocks:
            outs.append(jax.ShapeDtypeStruct((n * T, width), BF16))
            out_specs.append(ANY)
            if n_sendx:
                outs.append(jax.ShapeDtypeStruct((n_sendx * T, width), BF16))
                out_specs.append(ANY)
            scratch = [pltpu.VMEM((2, T, width), BF16)] + [pltpu.SemaphoreType.DMA((2,))] * 3
        if recvs:
            scratch.append(pltpu.SemaphoreType.DMA((len(recvs),)))
        flops = n * T * 2 * (704 * 512 + 784 * 1024 + 3 * 512 * 512) if blocks else 1000
        return pl.pallas_call(
            functools.partial(stage_kernel, n, n_sendx, len(recvs), y is not None, bool(blocks)),
            out_shape=outs,
            grid_spec=pltpu.PrefetchScalarGridSpec(
                num_scalar_prefetch=1, grid=(n,), in_specs=specs, out_specs=out_specs, scratch_shapes=scratch
            ),
            input_output_aliases=aliases,
            cost_estimate=pl.CostEstimate(flops=flops, bytes_accessed=n * T * 4096, transcendentals=0),
            compiler_params=PARAMS(dimension_semantics=("arbitrary",)),
            name=name,
        )(tab, *args)

    def local_step(latents, queries, lat_ln1, lat_wq, lat_wk, lat_wv, lat_wo, lat_ln2, lat_up, lat_down, dec_lnq, dec_lnkv, dec_wq, dec_wk, dec_wv, dec_wo, dec_ln, dec_up, dec_down, dec_out):
        n_items, n_lat, width = latents.shape
        n_query = queries.shape[1]
        t_idx, y_idx = lax.axis_index("tp"), lax.axis_index("sp")
        x_idx, c_idx = t_idx // 2, t_idx % 2

        def item(dx, dy, dc):
            return 4 * (x_idx ^ dx) + 2 * (y_idx ^ dy) + (c_idx ^ dc)

        def swap_core(a):
            return lax.ppermute(a, "tp", CORE)

        def swap_chip(a):
            return lax.ppermute(a, "tp", CHIP)

        def swap_sp(a):
            return lax.ppermute(a, "sp", [(0, 1), (1, 0)])

        def rows_first(w):
            return jnp.transpose(w, (1, 2, 0)).reshape(-1, width)

        pack = jnp.stack([rows_first(lat_wq), rows_first(lat_wk), rows_first(lat_wv), lat_wo.reshape(-1, width), lat_up.T, lat_down])
        pair = jnp.stack([pack, swap_chip(pack)])
        shards = jnp.concatenate([pair, swap_core(pair)])

        col = lambda g: g.reshape(-1, 1)
        queries_t = jnp.swapaxes(queries, 1, 2)
        z_own = lax.dynamic_index_in_dim(latents, item(0, 0, 0), 0, keepdims=False).T
        kv_w = (col(dec_lnkv), dec_wk, dec_wv, dec_wo)
        weights = (col(dec_lnq), dec_wq.T, col(dec_ln), dec_up.T, dec_down.T, dec_out)
        kv_shapes = [jax.ShapeDtypeStruct((n_lat, width), BF16), jax.ShapeDtypeStruct((width, n_lat), BF16)]
        z_new, k_own, vw_own = pl.pallas_call(
            latent_kernel,
            out_shape=[jax.ShapeDtypeStruct((width, n_lat), BF16), *kv_shapes],
            scratch_shapes=[pltpu.VMEM((width, n_lat), BF16)],
            cost_estimate=pl.CostEstimate(flops=5_000_000_000, bytes_accessed=10_000_000, transcendentals=0),
            compiler_params=PARAMS(),
            name="latent",
        )(z_own, shards, col(lat_ln1), col(lat_ln2), *kv_w)

        def kv_of(z):
            return pl.pallas_call(
                kv_kernel,
                out_shape=kv_shapes,
                cost_estimate=pl.CostEstimate(flops=1_200_000_000, bytes_accessed=4_000_000, transcendentals=0),
                compiler_params=PARAMS(),
                name="kv",
            )(z, *kv_w)

        z_y = swap_sp(z_new)
        z_x = swap_chip(z_new)
        z_d = swap_sp(z_x)

        y_shape = (n_items, n_query, width)

        def blocks(dx, dy, dc, first, count):
            return [(item(dx, dy, dc), first + b) for b in range(count)]

        def spread(rows, where, n):
            per = len(where) * T // n
            dest = []
            for s in range(n):
                b, off = divmod(s * per, T)
                dest.append((where[b][0], where[b][1] * T + off))
            return rows, dest

        run = functools.partial(stage, y_shape=y_shape, queries_t=queries_t, weights=weights)
        own = (k_own, vw_own)
        y, s1 = run("d1", None, blocks=blocks(0, 0, 0, 0, 2), kv=own, recvs=[])
        x1, p1 = swap_chip(s1), swap_core(s1)
        y, s2 = run("d2", y, blocks=blocks(0, 0, 0, 2, 2), kv=own, recvs=[])
        x2, p2 = swap_chip(s2), swap_core(s2)
        y, s3, sx3 = run("d3", y, blocks=blocks(0, 0, 0, 4, 4), kv=own, n_sendx=2, recvs=[spread(p1, blocks(0, 0, 1, 0, 2), 4)])
        x3, p3 = swap_chip(sx3), swap_core(s3)
        f1 = swap_core(x1)
        y, s4 = run("d4", y, blocks=blocks(0, 1, 0, 0, 8), kv=kv_of(z_y), recvs=[spread(p2, blocks(0, 0, 1, 2, 2), 8)])
        p4 = swap_core(s4)
        f2 = swap_core(x2)
        y, s5 = run("d5", y, blocks=blocks(1, 1, 0, 0, 8), kv=kv_of(z_d), recvs=[spread(p3, blocks(0, 0, 1, 4, 4), 8), spread(x1, blocks(1, 0, 0, 0, 2), 8), spread(f1, blocks(1, 0, 1, 0, 2), 8)])
        p5 = swap_core(s5)
        y, s6 = run("d6", y, blocks=blocks(1, 0, 0, 6, 2), kv=kv_of(z_x), recvs=[spread(p4, blocks(0, 1, 1, 0, 8), 2), spread(x2, blocks(1, 0, 0, 2, 2), 2), spread(f2, blocks(1, 0, 1, 2, 2), 2)])
        p6 = swap_core(s6)
        f3 = swap_core(x3)
        (y,) = run("last", y, blocks=[], kv=None, steps=4, recvs=[spread(p5, blocks(1, 1, 1, 0, 8), 4), spread(p6, blocks(1, 0, 1, 6, 2), 4), spread(x3, blocks(1, 0, 0, 4, 2), 4), spread(f3, blocks(1, 0, 1, 4, 2), 4)])
        return y

    return jax.shard_map(local_step, mesh=mesh, in_specs=in_specs, out_specs=P("dp", "sp", None), check_vma=False)
```
